256 devices in a mesh: phase: 16 (over y, x), line: 16 (over z, core).
Axes of the slice: x: 4, y: 4, z: 8, core: 2. Of those that a mesh axis runs over, the one named last changes fastest.
Arguments:
- signal: bfloat16 [16, 16, 8192, 256], P('phase', 'line'), may hold values from -8 to 8, as said below
- tap_gain: float32 [3, 256], replicated, may hold values from 0.3 to 1.2
Outputs:
- echoed: bfloat16 [16, 16, 8192, 256], P('phase', 'line')
The draws below stay inside these ranges and needn't reach their ends.
Inputs may be any that keep to these rules, and one draw needn't show every extreme that they name: signal holds numbers from -8 to 8.
All inputs are finite; a program needn't handle non-finite values.
Results may differ from the reference program's by a relative error of at most 0.0055.
Values may be sent and summed in bfloat16 or wider, within the bound.
No kernel may reach another device: no remote copies, remote signals or barrier semaphores. Data moves between devices by JAX's collectives and lax.ppermute only.
A program may use at most 64 MiB of HBM per device.

```python
import jax
import jax.numpy as jnp
from jax import lax

STEPS_DEV = 8192
CHANNELS = 256
SEGMENTS = 16
RECORDS = 16


def draw_signal(key, part):
    keys = jax.random.split(key, 2)
    loud = jnp.exp(jax.random.uniform(keys[0], (SEGMENTS, RECORDS, 1, CHANNELS), jnp.float32, -1.2, 1.2))
    noise = jax.random.normal(keys[1], (SEGMENTS, RECORDS, STEPS_DEV, CHANNELS), jnp.float32)
    return jnp.clip(loud * noise, -8.0, 8.0).astype(jnp.bfloat16)


def setup_inputs(seed: int = 0) -> dict:
    arg_keys = jax.random.split(jax.random.key(seed), 3)
    signal = draw_signal(jax.random.fold_in(arg_keys[2], 71), 0)
    tap_gain = jnp.clip(jax.random.uniform(arg_keys[1], (3, CHANNELS), jnp.float32, 0.3, 1.2), 0.3, 1.2)
    return {"signal": signal, "tap_gain": tap_gain}


def reference(signal, tap_gain):
    wide_in = signal.astype(jnp.float32)
    mixed = tap_gain[0] * wide_in + tap_gain[1] * jnp.roll(wide_in, 2, axis=0) + tap_gain[2] * jnp.roll(wide_in, 3, axis=0)
    power = lax.optimization_barrier(jnp.mean(mixed * mixed, axis=(0, 2), keepdims=True))
    echoed = (mixed * lax.rsqrt(power + 1e-05)).astype(jnp.bfloat16)
    return echoed
```

```python
import jax
import jax.numpy as jnp
from jax import lax
from jax.experimental import pallas as pl
from jax.experimental.pallas import tpu as pltpu
from jax.sharding import PartitionSpec as P


SIDE = 4
PARTS = (256, 512, 512, 512, 256)
TILE = 16
BLOCK = 128
VMEM = 16 * 1024 * 1024


def along(dx, dy, leave_out=None):
    pairs = []
    for y in range(SIDE):
        for x in range(SIDE):
            if x != leave_out:
                pairs.append((y * SIDE + x, (y + dy) % SIDE * SIDE + (x + dx) % SIDE))
    return pairs


def mix_kernel(col_ref, *refs):
    own, before = refs[:SIDE], refs[SIDE : 2 * SIDE]
    gain_ref, prev_ref = refs[2 * SIDE : 2 * SIDE + 2]
    outs, power_ref = refs[2 * SIDE + 2 : -1], refs[-1]
    rows, channels = own[0].shape

    @pl.when(pl.program_id(0) == 0)
    def _():
        power_ref[...] = prev_ref[...]

    g0, g1, g2 = (jnp.broadcast_to(gain_ref[k : k + 1, :], (TILE, channels)) for k in range(3))

    for k in range(SIDE):

        @pl.when(col_ref[0] == k)
        def _():
            def step(i, total):
                at = pl.ds(pl.multiple_of(i * TILE, TILE), TILE)
                now = [ref[at, :].astype(jnp.float32) for ref in own]
                ago = [
                    None if d == k else ref[at, :].astype(jnp.float32)
                    for d, ref in enumerate(before)
                ]
                for e in range(SIDE):
                    x = (k - e) % SIDE
                    two = (now if x >= 2 else ago)[(e + 2) % SIDE]
                    three = (now if x == 3 else ago)[(e + 3) % SIDE]
                    mixed = g0 * now[e] + g1 * two + g2 * three
                    outs[e][at, :] = mixed.astype(jnp.bfloat16)
                    total = total + mixed * mixed
                return total

            total = lax.fori_loop(0, rows // TILE, step, jnp.zeros((TILE, channels), jnp.float32))
            power_ref[...] += total[:8] + total[8:]


def mix(col, own, before, tap_gain, prev):
    rows, channels = own[0].shape
    block = pl.BlockSpec((BLOCK, channels), lambda i, col: (i, 0))
    whole = lambda a: pl.BlockSpec(a.shape, lambda i, col: (0,) * a.ndim)
    size = rows * channels * SIDE
    *mixed, power = pl.pallas_call(
        mix_kernel,
        grid_spec=pltpu.PrefetchScalarGridSpec(
            num_scalar_prefetch=1,
            grid=(rows // BLOCK,),
            in_specs=[block] * (2 * SIDE) + [whole(tap_gain), whole(prev)],
            out_specs=[block] * SIDE + [whole(prev)],
        ),
        out_shape=[jax.ShapeDtypeStruct(own[0].shape, jnp.bfloat16)] * SIDE
        + [jax.ShapeDtypeStruct(prev.shape, jnp.float32)],
        cost_estimate=pl.CostEstimate(flops=10 * size, bytes_accessed=6 * size, transcendentals=0),
        compiler_params=pltpu.CompilerParams(vmem_limit_bytes=VMEM),
        name="mix",
    )(col, *own, *before, tap_gain, prev)
    return mixed, power


def scale_kernel(steps, col_ref, *refs):
    sums, mixed, out_ref = refs[:SIDE], refs[SIDE : 2 * SIDE], refs[-1]
    power = sum(jnp.sum(ref[...], axis=0, keepdims=True) for ref in sums) / steps
    scale = lax.rsqrt(power + 1e-05)
    for e in range(SIDE):

        @pl.when(pl.program_id(0) == e)
        def _():
            out_ref[...] = (mixed[e][...].astype(jnp.float32) * scale).astype(jnp.bfloat16)


def scale(col, sums, mixed, start, steps, out):
    rows, channels = mixed[0].shape
    blocks = rows // BLOCK

    def walk(e):
        return lambda i, j, col: (jnp.where(i == e, j, jnp.where(i < e, 0, blocks - 1)), 0)

    whole = pl.BlockSpec(sums[0].shape, lambda i, j, col: (0, 0))
    size = rows * channels * SIDE
    into = [] if out is None else [out]
    per_hub = steps // (SIDE * SIDE * SIDE * BLOCK)
    return pl.pallas_call(
        lambda *refs: scale_kernel(steps, *refs),
        grid_spec=pltpu.PrefetchScalarGridSpec(
            num_scalar_prefetch=1,
            grid=(SIDE, blocks),
            in_specs=[whole] * SIDE
            + [pl.BlockSpec((BLOCK, channels), walk(e)) for e in range(SIDE)]
            + [pl.BlockSpec(memory_space=pl.ANY) for _ in into],
            out_specs=pl.BlockSpec(
                (BLOCK, channels),
                lambda i, j, col: (
                    lax.rem(col[0] + i, SIDE) * per_hub + start // BLOCK + j,
                    0,
                ),
            ),
        ),
        out_shape=jax.ShapeDtypeStruct((per_hub * BLOCK * SIDE, channels), jnp.bfloat16),
        input_output_aliases={1 + 2 * SIDE: 0} if into else {},
        cost_estimate=pl.CostEstimate(flops=2 * size, bytes_accessed=4 * size, transcendentals=0),
        compiler_params=pltpu.CompilerParams(vmem_limit_bytes=VMEM),
        name="scale",
    )(col, *sums, *mixed, *into)


def body(signal, tap_gain):
    steps, channels = signal.shape[2:]
    local = signal.reshape(steps, channels)
    slab = steps // SIDE
    where = lax.rem(lax.axis_index("phase"), SIDE)
    col = where.reshape(1)
    starts = [sum(PARTS[:c]) for c in range(len(PARTS))]

    def send(array, dx, dy, leave_out=None):
        return lax.ppermute(array, "phase", along(dx, dy, leave_out))

    power = jnp.zeros((8, channels), jnp.float32)
    back = []
    for start, rows in zip(starts, PARTS):
        own = []
        for d in range(SIDE):
            hub = lax.rem(where + d, SIDE)
            piece = lax.dynamic_slice(local, (hub * slab + start, 0), (rows, channels))
            own.append(send(piece, d, 0) if d else piece)
        before = []
        for d in range(SIDE):
            before.append(send(own[d], 0, 1, leave_out=d))
        mixed, power = mix(col, own, before, tap_gain, power)
        home = []
        for e in range(SIDE):
            home.append(send(mixed[e], -e, 0) if e else mixed[e])
        back.append(home)
    power = power + sum(send(power, 0, d) for d in range(1, SIDE))
    sums = [power] + [send(power, d, 0) for d in range(1, SIDE)]
    out = None
    for c, start in enumerate(starts):
        out = scale(col, sums, back[c], start, steps * SIDE * SIDE, out)
    return out.reshape(signal.shape)


def solution(mesh):
    return jax.shard_map(
        body,
        mesh=mesh,
        in_specs=(P("phase", "line", None, None), P()),
        out_specs=P("phase", "line", None, None),
        check_vma=False,
    )
```

```python
import jax
import jax.numpy as jnp
from jax import lax
from jax.experimental import pallas as pl
from jax.experimental.pallas import tpu as pltpu
from jax.sharding import PartitionSpec as P

TILE = 16
EXTRA = 16
VMEM = 24 * 1024 * 1024


def mix_kernel(chunk_ref, gain_ref, mixed_ref):
    segments, rows, channels = chunk_ref.shape
    g0, g1, g2 = (jnp.broadcast_to(gain_ref[k : k + 1, :], (TILE, channels)) for k in range(3))

    def step(i, total):
        at = pl.ds(pl.multiple_of(i * TILE, TILE), TILE)
        wide = [chunk_ref[s, at, :].astype(jnp.float32) for s in range(segments)]
        for s in range(segments):
            mixed = g0 * wide[s] + g1 * wide[s - 2] + g2 * wide[s - 3]
            mixed_ref[s, at, :] = mixed.astype(jnp.bfloat16)
            total = total + mixed * mixed
        return total

    total = lax.fori_loop(0, rows // TILE, step, jnp.zeros((TILE, channels), jnp.float32))
    power = jnp.sum(total, axis=0, keepdims=True)
    high = power.astype(jnp.bfloat16)
    rest = power - high.astype(jnp.float32)
    middle = rest.astype(jnp.bfloat16)
    low = (rest - middle.astype(jnp.float32)).astype(jnp.bfloat16)
    row = lax.broadcasted_iota(jnp.int32, (EXTRA, channels), 0)
    spread = lambda a: jnp.broadcast_to(a.astype(jnp.float32), (EXTRA, channels))
    terms = jnp.where(
        row == 0,
        spread(high),
        jnp.where(row == 1, spread(middle), jnp.where(row == 2, spread(low), 0.0)),
    ).astype(jnp.bfloat16)
    for s in range(segments):
        mixed_ref[s, pl.ds(rows, EXTRA), :] = terms


def mix(chunk, tap_gain):
    segments, rows, channels = chunk.shape
    return pl.pallas_call(
        mix_kernel,
        in_specs=[pl.BlockSpec(memory_space=pltpu.VMEM)] * 2,
        out_specs=pl.BlockSpec(memory_space=pltpu.VMEM),
        out_shape=jax.ShapeDtypeStruct((segments, rows + EXTRA, channels), jnp.bfloat16),
        cost_estimate=pl.CostEstimate(
            flops=10 * chunk.size, bytes_accessed=4 * chunk.size, transcendentals=0
        ),
        compiler_params=pltpu.CompilerParams(vmem_limit_bytes=VMEM),
        name="mix",
    )(chunk, tap_gain)


def scale_kernel(count, mixed_ref, out_ref, held, sems):
    segments, rows, channels = mixed_ref.shape
    rows -= EXTRA
    power = jnp.zeros((EXTRA, channels), jnp.float32)
    for s in range(segments):
        power = power + mixed_ref[s, pl.ds(rows, EXTRA), :].astype(jnp.float32)
    power = jnp.sum(power, axis=0, keepdims=True) / count
    scale = jnp.broadcast_to(lax.rsqrt(power + 1e-05), (TILE, channels))
    copies = []
    for s in range(segments):

        def step(i, carry):
            at = pl.ds(pl.multiple_of(i * TILE, TILE), TILE)
            held[s, at, :] = (mixed_ref[s, at, :].astype(jnp.float32) * scale).astype(jnp.bfloat16)
            return carry

        lax.fori_loop(0, rows // TILE, step, 0, unroll=4)
        copies.append(
            pltpu.make_async_copy(held.at[s], out_ref.at[pl.ds(s * rows, rows)], sems.at[s])
        )
        copies[-1].start()
    for copy in copies:
        copy.wait()


def scale(mixed, count):
    segments, rows, channels = mixed.shape
    rows -= EXTRA
    size = segments * rows * channels
    return pl.pallas_call(
        lambda *refs: scale_kernel(count, *refs),
        in_specs=[pl.BlockSpec(memory_space=pltpu.VMEM)],
        out_specs=pl.BlockSpec(memory_space=pl.ANY),
        out_shape=jax.ShapeDtypeStruct((segments * rows, channels), jnp.bfloat16),
        scratch_shapes=[
            pltpu.VMEM((segments, rows, channels), jnp.bfloat16),
            pltpu.SemaphoreType.DMA((segments,)),
        ],
        cost_estimate=pl.CostEstimate(flops=2 * size, bytes_accessed=4 * size, transcendentals=0),
        compiler_params=pltpu.CompilerParams(vmem_limit_bytes=VMEM),
        name="scale",
    )(mixed)


def body(signal, tap_gain):
    steps, channels = signal.shape[2:]
    peers = lax.axis_size("phase")
    pieces = signal.reshape(peers, steps // peers, channels)
    arrived = lax.all_to_all(pieces, "phase", split_axis=0, concat_axis=0, tiled=True)
    mixed = mix(arrived, tap_gain)
    home = lax.all_to_all(mixed, "phase", split_axis=0, concat_axis=0, tiled=True)
    return scale(home, steps * peers).reshape(signal.shape)


def solution(mesh):
    return jax.shard_map(
        body,
        mesh=mesh,
        in_specs=(P("phase", "line", None, None), P()),
        out_specs=P("phase", "line", None, None),
        check_vma=False,
    )
```
